32 devices in a mesh: seq: 8 (over y, x, core), head: 4 (over z).
Axes of the slice: x: 2, y: 2, z: 4, core: 2. Of those that a mesh axis runs over, the one named last changes fastest.
Arguments:
- queries: bfloat16 [2048, 2048], P('seq', 'head'), may hold values from -24 to 24
- key_vectors: bfloat16 [2048, 512], P('seq', 'head'), may hold values from -4 to 4
- values: bfloat16 [2048, 512], P('seq', 'head'), may hold values from -6 to 6
- out_proj: bfloat16 [2048, 4096], P('head'), may hold values from -0.125 to 0.125
- grad_out: bfloat16 [2048, 4096], P('seq', 'head'), may hold values from -6 to 6
- windows: int32 [16], P('head'), may hold values from 512 to 1024, as said below
- slab_order: int32 [8], replicated, may hold values from 0 to 7, as said below
Outputs:
- layer_out: bfloat16 [2048, 4096], P('seq', 'head')
- grad_queries: bfloat16 [2048, 2048], P('seq', 'head')
- grad_keys: bfloat16 [2048, 512], P('seq', 'head')
- grad_values: bfloat16 [2048, 512], P('seq', 'head')
The draws below stay inside these ranges and needn't reach their ends.
Inputs may be any that keep to these rules, and one draw needn't show every extreme that they name: `windows`: some head's window is exactly 1024. slab_order[d] = (d + c) mod 8 for one c with 0 <= c < 8.
All inputs are finite; a program needn't handle non-finite values.
Results may differ from the reference program's by a relative error of at most 0.019.
Values may be sent and summed in bfloat16 or wider, within the bound.
No kernel may reach another device: no remote copies, remote signals or barrier semaphores. Data moves between devices by JAX's collectives and lax.ppermute only.
A program may use at most 128 MiB of HBM per device.

```python
import jax
import jax.numpy as jnp
from jax import lax

MODEL_DIM = 4096
HEADS = 16
KV_HEADS = 4
HEAD_DIM = 128
TOK_DEV = 256
SLABS = 8
TOKENS = 2048
WIN_SLABS = 4
WINDOW = 1024
HEAD_SETS = 4


def drawn_pair(key):
    base = jax.random.fold_in(key, 7301)
    key_query, key_key = jax.random.split(base, 2)
    queries = 2.5 * jax.random.truncated_normal(key_query, -3.2, 3.2, (TOKENS, HEADS * HEAD_DIM), jnp.float32)
    key_vectors = jax.random.truncated_normal(key_key, -4.0, 4.0, (TOKENS, KV_HEADS * HEAD_DIM), jnp.float32)
    return (queries, key_vectors)


def draw_queries(key, part):
    return drawn_pair(key)[0].astype(jnp.bfloat16)


def draw_key_vectors(key, part):
    return drawn_pair(key)[1].astype(jnp.bfloat16)


def draw_windows(key, part):
    base = jax.random.fold_in(key, 4409)
    key_length, key_head = jax.random.split(base)
    lengths = jax.random.randint(key_length, (HEADS,), WINDOW // 2, WINDOW + 1)
    chosen = jax.random.randint(key_head, (), 0, HEADS)
    return jnp.where(jnp.arange(HEADS) == chosen, WINDOW, lengths).astype(jnp.int32)


def draw_slab_order(key, part):
    shift_by = jax.random.randint(jax.random.fold_in(key, 90211), (), 0, SLABS)
    return jnp.mod(jnp.arange(SLABS, dtype=jnp.int32) + shift_by, SLABS).astype(jnp.int32)


def shard_levels(own_key, extent, cuts, low, high):
    factor_of = 1.0
    for dim, shards_of in cuts:
        steps = jax.random.uniform(jax.random.fold_in(jax.random.fold_in(own_key, 6), dim), (shards_of,), jnp.float32, low / len(cuts), high / len(cuts))
        factor_of = factor_of * jnp.repeat(jnp.exp(steps), extent[dim] // shards_of).reshape((-1,) + (1,) * (len(extent) - 1 - dim))
    return factor_of


def scatter_about(rng, extent, deviation, bound, pieces=(), kind=jnp.bfloat16):
    factor_of = shard_levels(rng, extent, pieces, -0.22, 0.18) if pieces else 1.0
    values = jax.random.normal(rng, extent, jnp.float32) * deviation * factor_of
    return jnp.minimum(jnp.maximum(values, -bound), bound).astype(kind)


def setup_inputs(seed: int = 0) -> dict:
    streams_of = jax.random.split(jax.random.key(seed), 8)
    queries = draw_queries(jax.random.fold_in(streams_of[7], 71), 0)
    key_vectors = draw_key_vectors(jax.random.fold_in(streams_of[7], 71), 0)
    values = scatter_about(streams_of[2], (TOKENS, KV_HEADS * HEAD_DIM), 1.0, 6.0, ((0, 8), (1, 4)))
    out_proj = scatter_about(streams_of[3], (HEADS * HEAD_DIM, MODEL_DIM), (HEADS * HEAD_DIM) ** -0.5, 0.125, ((0, 4),))
    grad_out = scatter_about(streams_of[4], (TOKENS, MODEL_DIM), 1.0, 6.0, ((0, 8), (1, 4)))
    windows = draw_windows(jax.random.fold_in(streams_of[7], 71), 0)
    slab_order = draw_slab_order(jax.random.fold_in(streams_of[7], 71), 0)
    return {"queries": queries, "key_vectors": key_vectors, "values": values, "out_proj": out_proj, "grad_out": grad_out, "windows": windows, "slab_order": slab_order}


LOWEST = -1.0e30


def reference(queries, key_vectors, values, out_proj, grad_out, windows, slab_order):
    rows = TOK_DEV
    slabs = SLABS
    reach = WIN_SLABS
    span = (reach + 1) * rows
    groups = KV_HEADS
    ratio = HEADS // KV_HEADS
    scale = HEAD_DIM ** -0.5
    inverse = jnp.zeros((slabs,), jnp.int32).at[slab_order].set(jnp.arange(slabs, dtype=jnp.int32))

    def order(array):
        return array.reshape(slabs, rows, array.shape[1])[inverse].reshape(TOKENS, array.shape[1])

    def restore(array):
        return array.reshape(slabs, rows, array.shape[-1])[slab_order].reshape(TOKENS, array.shape[-1])

    grad_attn = jnp.dot(grad_out, out_proj.T, preferred_element_type=jnp.float32).astype(jnp.bfloat16)
    query_sorted = order(queries)
    grad_sorted = order(grad_attn)
    padding = jnp.zeros((reach * rows, groups * HEAD_DIM), jnp.bfloat16)
    key_padded = jnp.concatenate([padding, order(key_vectors)], 0)
    value_padded = jnp.concatenate([padding, order(values)], 0)
    spans = windows.reshape(groups, ratio)[:, :, None, None]
    offsets = jnp.arange(rows, dtype=jnp.int32)
    key_offsets = jnp.arange(span, dtype=jnp.int32)

    def one_slab(carry, slab):
        key_grads, value_grads = carry
        start = (slab * rows).astype(jnp.int32)
        query_heads = lax.dynamic_slice_in_dim(query_sorted, start, rows, 0).reshape(rows, groups, ratio, HEAD_DIM).astype(jnp.float32)
        grad_heads = lax.dynamic_slice_in_dim(grad_sorted, start, rows, 0).reshape(rows, groups, ratio, HEAD_DIM).astype(jnp.float32)
        key_heads = lax.dynamic_slice_in_dim(key_padded, start, span, 0).reshape(span, groups, HEAD_DIM).astype(jnp.float32)
        value_heads = lax.dynamic_slice_in_dim(value_padded, start, span, 0).reshape(span, groups, HEAD_DIM).astype(jnp.float32)
        query_place = start + offsets
        key_place = start - reach * rows + key_offsets
        distance = query_place[:, None] - key_place[None, :]
        mask = (distance >= 0) & (distance < spans) & (key_place >= 0)[None, :]
        scores = jnp.einsum("igrd,jgd->grij", query_heads, key_heads) * scale
        peak = jnp.max(jnp.where(mask, scores, LOWEST), -1)
        total = jnp.sum(jnp.exp(jnp.where(mask, scores - peak[..., None], LOWEST)), -1)
        log_norm = peak + jnp.log(total)
        probs = jnp.exp(jnp.where(mask, scores - log_norm[..., None], LOWEST))
        rounded = lax.optimization_barrier(probs.astype(jnp.bfloat16)).astype(jnp.float32)
        attention = jnp.einsum("grij,jgd->igrd", rounded, value_heads).astype(jnp.bfloat16)
        attention_wide = lax.optimization_barrier(attention).astype(jnp.float32)
        delta = jnp.einsum("igrd,igrd->gri", grad_heads, attention_wide)
        grad_prob = jnp.einsum("igrd,jgd->grij", grad_heads, value_heads)
        grad_score = (probs * (grad_prob - delta[..., None]) * scale).astype(jnp.bfloat16)
        grad_score = lax.optimization_barrier(grad_score).astype(jnp.float32)
        grad_q = jnp.einsum("grij,jgd->igrd", grad_score, key_heads)
        grad_k = jnp.einsum("grij,igrd->jgd", grad_score, query_heads).reshape(span, groups * HEAD_DIM)
        grad_v = jnp.einsum("grij,igrd->jgd", rounded, grad_heads).reshape(span, groups * HEAD_DIM)
        key_grads = lax.dynamic_update_slice_in_dim(key_grads, lax.dynamic_slice_in_dim(key_grads, start, span, 0) + grad_k, start, 0)
        value_grads = lax.dynamic_update_slice_in_dim(value_grads, lax.dynamic_slice_in_dim(value_grads, start, span, 0) + grad_v, start, 0)
        return (key_grads, value_grads), (attention.reshape(rows, HEADS * HEAD_DIM), grad_q.reshape(rows, HEADS * HEAD_DIM).astype(jnp.bfloat16))

    start_grads = jnp.zeros(((slabs + reach) * rows, groups * HEAD_DIM), jnp.float32)
    (key_grads, value_grads), (attention_sorted, grad_q_sorted) = lax.scan(one_slab, (start_grads, start_grads), jnp.arange(slabs, dtype=jnp.int32))
    attention = restore(attention_sorted)
    grad_queries = restore(grad_q_sorted)
    grad_keys = restore(key_grads[reach * rows:]).astype(jnp.bfloat16)
    grad_values = restore(value_grads[reach * rows:]).astype(jnp.bfloat16)
    width = HEADS * HEAD_DIM // HEAD_SETS
    summed = jnp.zeros((TOKENS, MODEL_DIM), jnp.float32)
    for member in range(HEAD_SETS):
        share = jnp.dot(attention[:, member * width:(member + 1) * width], out_proj[member * width:(member + 1) * width], preferred_element_type=jnp.float32)
        summed = summed + lax.optimization_barrier(share.astype(jnp.bfloat16)).astype(jnp.float32)
    layer_out = summed.astype(jnp.bfloat16)
    return layer_out, grad_queries, grad_keys, grad_values
```

```python
import functools

import jax
import jax.numpy as jnp
from jax import lax
from jax.experimental import pallas as pl
from jax.experimental.pallas import tpu as pltpu
from jax.sharding import PartitionSpec as P

HEAD_DIM = 128
LOWEST = -1e30
LOG2_E = 1.4426950408889634
F32 = jnp.float32
BF16 = jnp.bfloat16

NT = (((1,), (1,)), ((), ()))
NN = (((1,), (0,)), ((), ()))

WHOLE = pl.BlockSpec(memory_space=pltpu.VMEM)
MAIN = pl.BlockSpec(memory_space=pltpu.HBM)
PARAMS = pltpu.CompilerParams(vmem_limit_bytes=24 * 1024 * 1024)


def dot(a, b, dims=NN):
    return lax.dot_general(a, b, dims, preferred_element_type=F32)


def head_of(array, index):
    return array[:, index * HEAD_DIM : (index + 1) * HEAD_DIM]


def columns_at(proj, index, share):
    return proj.at[:, pl.ds(pl.multiple_of(index * share, share), share)]


def main(array):
    return pltpu.with_memory_space_constraint(array, pltpu.HBM)


def estimate(flops, size):
    return pl.CostEstimate(flops=flops, bytes_accessed=size, transcendentals=0)


def stage_kernel(keys, values, queries, windows, order, pair, query, limits, spans, slabs, sems, *, reach):
    rows, width = keys.shape
    copies = [
        pltpu.make_async_copy(windows, spans, sems.at[0]),
        pltpu.make_async_copy(order, slabs, sems.at[1]),
        pltpu.make_async_copy(keys, pair.at[:, pl.ds(0, width)], sems.at[2]),
        pltpu.make_async_copy(values, pair.at[:, pl.ds(width, width)], sems.at[3]),
        pltpu.make_async_copy(queries, query, sems.at[4]),
    ]
    for copy in copies:
        copy.start()
    copies[0].wait()
    copies[1].wait()
    slab = slabs[lax.axis_index("seq")]
    for head in range(windows.shape[0]):
        for step in range(reach + 1):
            limit = jnp.where(slab >= step, spans[head] - step * rows, -rows)
            limits[pl.ds(head * (reach + 1) + step, 1), :] = jnp.full((1, rows), limit, jnp.int32)
    for copy in copies[2:]:
        copy.wait()


def stage(key_vectors, values, queries, windows, slab_order, reach):
    rows, width = key_vectors.shape
    heads = windows.shape[0]
    return pl.pallas_call(
        functools.partial(stage_kernel, reach=reach),
        in_specs=[MAIN] * 5,
        out_specs=[WHOLE] * 3,
        out_shape=[
            pltpu.VMEM((rows, 2 * width), BF16),
            pltpu.VMEM(queries.shape, BF16),
            pltpu.VMEM((heads * (reach + 1), rows), jnp.int32),
        ],
        scratch_shapes=[
            pltpu.SMEM(windows.shape, jnp.int32),
            pltpu.SMEM(slab_order.shape, jnp.int32),
            pltpu.SemaphoreType.DMA((5,)),
        ],
        compiler_params=PARAMS,
        cost_estimate=estimate(rows * width, 8 * rows * width),
        name="stage",
    )(*[main(array) for array in (key_vectors, values, queries, windows, slab_order)])


def forward_kernel(limits, query, proj, *refs, reach, groups):
    blocks = refs[: reach + 1]
    attention, turned, probs, lead, local = refs[reach + 1 : reach + 6]
    (sem,) = refs[reach + 6 :]
    rows, width = query.shape
    heads = width // HEAD_DIM
    size = lax.axis_size("head")
    place = size - 1 - lax.axis_index("head")
    copy = pltpu.make_async_copy(proj, local, sem)
    copy.start()
    scale = HEAD_DIM ** (-0.5) * LOG2_E
    offset = lax.broadcasted_iota(jnp.int32, (rows, rows), 1) - lax.broadcasted_iota(
        jnp.int32, (rows, rows), 0
    )
    turned_values = [
        [head_of(blocks[step], groups + group).T for step in range(reach + 1)]
        for group in range(groups)
    ]

    def head_scores(head):
        scores = []
        for step in range(reach + 1):
            score = dot(head_of(blocks[step], head * groups // heads), head_of(query, head), NT)
            mask = offset < limits[pl.ds(head * (reach + 1) + step, 1), :]
            if step == 0:
                mask = mask & (offset >= 0)
            scores.append(jnp.where(mask, score, LOWEST))
        return scores

    scores = head_scores(0)
    for head in range(heads):
        following = head_scores(head + 1) if head + 1 < heads else None
        peak = functools.reduce(
            jnp.maximum, [jnp.max(score, 0, keepdims=True) for score in scores]
        )
        powers = [jnp.exp2((score - peak) * scale) for score in scores]
        inverse = 1.0 / sum(jnp.sum(power, 0, keepdims=True) for power in powers)
        mixed = jnp.zeros((HEAD_DIM, rows), F32)
        for step in range(reach + 1):
            prob = (powers[step] * inverse).astype(BF16)
            probs[pl.ds(step * rows, rows), pl.ds(head * rows, rows)] = prob
            mixed = mixed + dot(turned_values[head * groups // heads][step], prob)
        turned[pl.ds(head * HEAD_DIM, HEAD_DIM), :] = mixed.astype(BF16)
        attention[:, pl.ds(head * HEAD_DIM, HEAD_DIM)] = mixed.T.astype(BF16)
        scores = following
    copy.wait()
    lead[0] = dot(attention[...], columns_at(local, place, lead.shape[2])[...]).astype(BF16)


def forward(limits, query, out_proj, blocks, groups, size):
    rows, width = query.shape
    heads = width // HEAD_DIM
    reach = len(blocks) - 1
    share = out_proj.shape[1] // size
    span = (reach + 1) * rows
    return pl.pallas_call(
        functools.partial(forward_kernel, reach=reach, groups=groups),
        in_specs=[WHOLE, WHOLE, MAIN] + [WHOLE] * (reach + 1),
        out_specs=[WHOLE] * 5,
        out_shape=[
            pltpu.VMEM((rows, width), BF16),
            pltpu.VMEM((width, rows), BF16),
            pltpu.VMEM((span, heads * rows), BF16),
            pltpu.VMEM((1, rows, share), BF16),
            pltpu.VMEM(out_proj.shape, BF16),
        ],
        scratch_shapes=[pltpu.SemaphoreType.DMA],
        compiler_params=PARAMS,
        cost_estimate=estimate(4 * rows * span * width, 8 * rows * span),
        name="forward",
    )(limits, query, main(out_proj), *blocks)


def send_kernel(shares, passed, out, *, end, inner):
    z = lax.axis_index("head")

    @pl.when(z == end)
    def _():
        out[...] = shares[0]

    if inner is None:

        @pl.when(z != end)
        def _():
            out[...] = passed[...]

    else:

        @pl.when(z == inner)
        def _():
            out[...] = passed[...]

        @pl.when((z != end) & (z != inner))
        def _():
            out[...] = shares[0] + passed[...]


def send(shares, passed, end, inner, name):
    return pl.pallas_call(
        functools.partial(send_kernel, end=end, inner=inner),
        in_specs=[WHOLE] * 2,
        out_specs=WHOLE,
        out_shape=pltpu.VMEM(passed.shape, BF16),
        compiler_params=PARAMS,
        cost_estimate=estimate(passed.size, 6 * passed.size),
        name=name,
    )(shares, passed)


def middle_kernel(attention, own, above, below, proj, shares, partial, extra, sem):
    size = lax.axis_size("head")
    z = lax.axis_index("head")
    share = extra.shape[1]
    copy = pltpu.make_async_copy(own, extra, sem)
    copy.start()
    places = [lax.rem(z + size // 2, size), jnp.minimum(z + 1, size - 1), jnp.maximum(z - 1, 0), z]
    total = None
    for slot, source in enumerate((None, below, above, extra)):
        block = columns_at(proj, places[slot], share)[...]
        shares[slot] = dot(attention[...], block).astype(BF16)
        if source is extra:
            copy.wait()
        if source is not None:
            part = dot(block, source[...], NT)
            total = part if total is None else total + part
    partial[...] = total


def middle(attention, own, above, below, out_proj, size):
    rows, width = attention.shape
    share = out_proj.shape[1] // size
    return pl.pallas_call(
        middle_kernel,
        in_specs=[WHOLE, MAIN, WHOLE, WHOLE, WHOLE],
        out_specs=[WHOLE] * 2,
        out_shape=[
            pltpu.VMEM((4, rows, share), BF16),
            pltpu.VMEM((width, rows), F32),
        ],
        scratch_shapes=[pltpu.VMEM(own.shape, BF16), pltpu.SemaphoreType.DMA],
        compiler_params=PARAMS,
        cost_estimate=estimate(14 * rows * share * width, 8 * share * width),
        name="middle",
    )(attention, main(own), above, below, out_proj)


def far_kernel(partial, above, below, proj, out):
    size = lax.axis_size("head")
    z = lax.axis_index("head")
    share = above.shape[1]
    block = columns_at(proj, lax.rem(z + size // 2, size), share)

    @pl.when(z >= size // 2)
    def _():
        out[...] = partial[...] + dot(block[...], above[...], NT)

    @pl.when(z < size // 2)
    def _():
        out[...] = partial[...] + dot(block[...], below[...], NT)


def far(partial, above, below, out_proj):
    rows, share = above.shape
    width = out_proj.shape[0]
    return pl.pallas_call(
        far_kernel,
        in_specs=[WHOLE] * 4,
        out_specs=WHOLE,
        out_shape=pltpu.VMEM((width, rows), F32),
        compiler_params=PARAMS,
        cost_estimate=estimate(2 * rows * share * width, 2 * share * width),
        name="far",
    )(partial, above, below, out_proj)


def backward_kernel(partial, above, below, query, turned, probs, proj, *refs, reach, groups):
    blocks = refs[: reach + 1]
    grads = refs[reach + 1 : 2 * reach + 1]
    scores, ups, upstream = refs[2 * reach + 1 :]
    rows, width = query.shape
    heads = width // HEAD_DIM
    ratio = heads // groups
    size = lax.axis_size("head")
    z = lax.axis_index("head")
    share = above.shape[1]
    scale = HEAD_DIM ** (-0.5)
    block = columns_at(proj, size - 1 - z, share)

    @pl.when(z == size - 1)
    def _():
        upstream[...] = (partial[...] + dot(block[...], above[...], NT)).astype(BF16)

    @pl.when(z == 0)
    def _():
        upstream[...] = (partial[...] + dot(block[...], below[...], NT)).astype(BF16)

    @pl.when((z > 0) & (z < size - 1))
    def _():
        upstream[...] = partial[...].astype(BF16)

    for head in range(heads):
        up = upstream[pl.ds(head * HEAD_DIM, HEAD_DIM), :]
        ups[pl.ds(head * rows, rows), :] = up.T
        wide = up.astype(F32) * turned[pl.ds(head * HEAD_DIM, HEAD_DIM), :].astype(F32)
        delta = jnp.sum(wide, 0, keepdims=True)
        columns = pl.ds(head * rows, rows)
        for step in range(reach + 1):
            spot = pl.ds(step * rows, rows)
            grad_prob = dot(head_of(blocks[step], groups + head // ratio), up)
            scores[spot, columns] = (
                probs[spot, columns].astype(F32) * (grad_prob - delta)
            ).astype(BF16)
    for group in range(groups):
        tall_query = jnp.concatenate(
            [head_of(query, head) for head in range(group * ratio, (group + 1) * ratio)], 0
        )
        columns = pl.ds(group * ratio * rows, ratio * rows)
        for step in range(1, reach + 1):
            spot = pl.ds(step * rows, rows)
            grads[step - 1][:, pl.ds(group * HEAD_DIM, HEAD_DIM)] = (
                dot(scores[spot, columns], tall_query) * scale
            ).astype(BF16)
            grads[step - 1][:, pl.ds((groups + group) * HEAD_DIM, HEAD_DIM)] = dot(
                probs[spot, columns], ups[columns, :]
            ).astype(BF16)


def backward(partial, above, below, query, turned, probs, out_proj, blocks, groups):
    rows, width = query.shape
    heads = width // HEAD_DIM
    reach = len(blocks) - 1
    span = (reach + 1) * rows
    outs = pl.pallas_call(
        functools.partial(backward_kernel, reach=reach, groups=groups),
        in_specs=[WHOLE] * (reach + 8),
        out_specs=[WHOLE] * (reach + 2),
        out_shape=[pltpu.VMEM((rows, 2 * groups * HEAD_DIM), BF16)] * reach
        + [
            pltpu.VMEM(probs.shape, BF16),
            pltpu.VMEM((heads * rows, HEAD_DIM), BF16),
        ],
        scratch_shapes=[pltpu.VMEM((width, rows), BF16)],
        compiler_params=PARAMS,
        cost_estimate=estimate(8 * rows * span * width, 8 * rows * span),
        name="backward",
    )(partial, above, below, query, turned, probs, out_proj, *blocks)
    return outs[:reach], outs[reach], outs[reach + 1]


def finish_kernel(scores, ups, query, probs, *refs, reach, groups):
    blocks = refs[: reach + 1]
    grad_query, grad = refs[reach + 1 :]
    rows, width = query.shape
    heads = width // HEAD_DIM
    ratio = heads // groups
    scale = HEAD_DIM ** (-0.5)
    spot = pl.ds(0, rows)
    for group in range(groups):
        picked = range(group * ratio, (group + 1) * ratio)
        tall_query = jnp.concatenate([head_of(query, head) for head in picked], 0)
        columns = pl.ds(group * ratio * rows, ratio * rows)
        grad[:, pl.ds(group * HEAD_DIM, HEAD_DIM)] = dot(scores[spot, columns], tall_query) * scale
        grad[:, pl.ds((groups + group) * HEAD_DIM, HEAD_DIM)] = dot(
            probs[spot, columns], ups[columns, :]
        )
        keys = jnp.concatenate([head_of(blocks[step], group) for step in range(reach + 1)], 0).T
        for head in picked:
            total = dot(keys, scores[:, pl.ds(head * rows, rows)])
            grad_query[:, pl.ds(head * HEAD_DIM, HEAD_DIM)] = (total * scale).T.astype(BF16)


def finish(scores, ups, query, probs, blocks, groups):
    rows, width = query.shape
    reach = len(blocks) - 1
    span = (reach + 1) * rows
    return pl.pallas_call(
        functools.partial(finish_kernel, reach=reach, groups=groups),
        in_specs=[WHOLE] * (reach + 5),
        out_specs=[WHOLE] * 2,
        out_shape=[
            jax.ShapeDtypeStruct((rows, width), BF16),
            pltpu.VMEM((rows, 2 * groups * HEAD_DIM), F32),
        ],
        compiler_params=PARAMS,
        cost_estimate=estimate(2 * rows * span * width, 4 * rows * span),
        name="finish",
    )(scores, ups, query, probs, *blocks)


def body(queries, key_vectors, values, out_proj, grad_out, windows, slab_order):
    groups = key_vectors.shape[1] // HEAD_DIM
    devices = lax.axis_size("seq")
    size = lax.axis_size("head")
    assert size == 4 and devices % 4 == 0
    reach = min(8, devices // 2)
    half = reach // 2
    even = lax.axis_index("seq") % 2 == 0
    nothing = jnp.zeros((), BF16)

    def climb(array):
        return lax.ppermute(array, "head", [(i, i + 1) for i in range(size - 1)])

    def descend(array):
        return lax.ppermute(array, "head", [(i + 1, i) for i in range(size - 1)])

    def shifted(array, step):
        return lax.ppermute(array, "seq", [((i - step) % devices, i) for i in range(devices)])

    def swapped(array):
        return lax.ppermute(array, "seq", [(i ^ 1, i) for i in range(devices)])

    pair, query, limits = stage(key_vectors, values, queries, windows, slab_order, reach)
    fetched = [pair] + [shifted(pair, 2 * step) for step in range(1, half + 1)]
    traded = [swapped(jnp.where(even, pair, fetched[half]))]
    traded += [swapped(fetched[step]) for step in range(1, half)]
    blocks = [pair]
    for step in range(half):
        blocks.append(jnp.where(even, traded[(step + 1) % half], traded[step]))
        blocks.append(fetched[step + 1])

    above1, below1 = climb(grad_out), descend(grad_out)
    attention, turned, probs, lead, proj = forward(limits, query, out_proj, blocks, groups, size)

    above2 = climb(send(lead, above1, 0, None, "send_up2"))
    below2 = descend(send(lead, below1, size - 1, None, "send_down2"))
    rest, partial = middle(attention, grad_out, above1, below1, proj, size)

    above3 = climb(send(rest, above2, 0, size // 2, "send_up3"))
    below3 = descend(send(rest, below2, size - 1, size // 2 - 1, "send_down3"))
    partial = far(partial, above2, below2, proj)

    sent, scores, ups = backward(
        partial, above3, below3, query, turned, probs, proj, blocks, groups
    )
    above4 = climb(rest[1] + above3)
    below4 = descend(rest[2] + below3)

    taken = [swapped(sent[2 * step]) for step in range(half)]
    total = []
    for step in range(half):
        near = taken[step]
        if step + 1 < half:
            near = jnp.where(even, taken[step + 1], near)
        else:
            near = jnp.where(even, nothing, near)
        total.append(shifted(sent[2 * step + 1] + near, -2 * (step + 1)))
    grad_queries, own = finish(scores, ups, query, probs, blocks, groups)
    own = own + jnp.where(even, taken[0], nothing).astype(F32)
    for part in total:
        own = own + part.astype(F32)
    grad_keys = own[:, : groups * HEAD_DIM].astype(BF16)
    grad_values = own[:, groups * HEAD_DIM :].astype(BF16)
    layer_out = (rest[3].astype(F32) + above4.astype(F32) + below4.astype(F32)).astype(BF16)
    return layer_out, grad_queries, grad_keys, grad_values


def solution(mesh):
    in_specs = (
        P("seq", "head"),
        P("seq", "head"),
        P("seq", "head"),
        P("head", None),
        P("seq", "head"),
        P("head"),
        P(),
    )
    out_specs = (P("seq", "head"), P("seq", "head"), P("seq", "head"), P("seq", "head"))
    return jax.shard_map(body, mesh=mesh, in_specs=in_specs, out_specs=out_specs, check_vma=False)
```

```python
import functools

import jax
import jax.numpy as jnp
from jax import lax
from jax.experimental import pallas as pl
from jax.experimental.pallas import tpu as pltpu
from jax.sharding import PartitionSpec as P


HEAD_DIM = 128
LOWEST = -1e30
LOG2_E = 1.4426950408889634
F32 = jnp.float32
BF16 = jnp.bfloat16

NT = (((1,), (1,)), ((), ()))
NN = (((1,), (0,)), ((), ()))

WHOLE = pl.BlockSpec(memory_space=pltpu.VMEM)
MAIN = pl.BlockSpec(memory_space=pltpu.HBM)
PARAMS = pltpu.CompilerParams(vmem_limit_bytes=24 * 1024 * 1024)


def dot(a, b, dims=NN):
    return lax.dot_general(a, b, dims, preferred_element_type=F32)


def head_of(array, index):
    return array[:, index * HEAD_DIM : (index + 1) * HEAD_DIM]


def columns_at(proj, index, share):
    return proj.at[:, pl.ds(pl.multiple_of(index * share, share), share)]


PARTS = 2


def parts_of(rows, width):
    return [pltpu.VMEM((rows // PARTS, width), BF16)] * PARTS


def in_parts(refs, whole):
    rows = refs[0].shape[0]
    for index, ref in enumerate(refs):
        ref[...] = whole[index * rows : (index + 1) * rows].astype(BF16)


def main(array):
    return pltpu.with_memory_space_constraint(array, pltpu.HBM)


def estimate(flops, size):
    return pl.CostEstimate(flops=flops, bytes_accessed=size, transcendentals=0)


def stage_kernel(keys, values, queries, windows, order, pair, query, limits, spans, slabs, sems, *, reach):
    rows, width = keys.shape
    copies = [
        pltpu.make_async_copy(windows, spans, sems.at[0]),
        pltpu.make_async_copy(order, slabs, sems.at[1]),
        pltpu.make_async_copy(keys, pair.at[:, pl.ds(0, width)], sems.at[2]),
        pltpu.make_async_copy(values, pair.at[:, pl.ds(width, width)], sems.at[3]),
        pltpu.make_async_copy(queries, query, sems.at[4]),
    ]
    for copy in copies:
        copy.start()
    copies[0].wait()
    copies[1].wait()
    slab = slabs[lax.axis_index("seq")]
    for head in range(windows.shape[0]):
        for step in range(reach + 1):
            limit = jnp.where(slab >= step, spans[head] - step * rows, -rows)
            limits[pl.ds(head * (reach + 1) + step, 1), :] = jnp.full((1, rows), limit, jnp.int32)
    for copy in copies[2:]:
        copy.wait()


def stage(key_vectors, values, queries, windows, slab_order, reach):
    rows, width = key_vectors.shape
    heads = windows.shape[0]
    return pl.pallas_call(
        functools.partial(stage_kernel, reach=reach),
        in_specs=[MAIN] * 5,
        out_specs=[WHOLE] * 3,
        out_shape=[
            pltpu.VMEM((rows, 2 * width), BF16),
            pltpu.VMEM(queries.shape, BF16),
            pltpu.VMEM((heads * (reach + 1), rows), jnp.int32),
        ],
        scratch_shapes=[
            pltpu.SMEM(windows.shape, jnp.int32),
            pltpu.SMEM(slab_order.shape, jnp.int32),
            pltpu.SemaphoreType.DMA((5,)),
        ],
        compiler_params=PARAMS,
        cost_estimate=estimate(rows * width, 8 * rows * width),
        name="stage",
    )(*[main(array) for array in (key_vectors, values, queries, windows, slab_order)])


def forward_kernel(limits, query, proj, *refs, reach, groups):
    blocks = refs[: reach + 1]
    attention, turned, probs, local = refs[reach + 1 : reach + 5]
    leads, sem = refs[reach + 5 : -1], refs[-1]
    rows, width = query.shape
    heads = width // HEAD_DIM
    size = lax.axis_size("head")
    place = size - 1 - lax.axis_index("head")
    copy = pltpu.make_async_copy(proj, local, sem)
    copy.start()
    scale = HEAD_DIM ** (-0.5) * LOG2_E
    offset = lax.broadcasted_iota(jnp.int32, (rows, rows), 1) - lax.broadcasted_iota(
        jnp.int32, (rows, rows), 0
    )
    turned_values = [
        [head_of(blocks[step], groups + group).T for step in range(reach + 1)]
        for group in range(groups)
    ]

    def head_scores(head):
        scores = []
        for step in range(reach + 1):
            score = dot(head_of(blocks[step], head * groups // heads), head_of(query, head), NT)
            mask = offset < limits[pl.ds(head * (reach + 1) + step, 1), :]
            if step == 0:
                mask = mask & (offset >= 0)
            scores.append(jnp.where(mask, score, LOWEST))
        return scores

    scores = head_scores(0)
    for head in range(heads):
        following = head_scores(head + 1) if head + 1 < heads else None
        peak = functools.reduce(
            jnp.maximum, [jnp.max(score, 0, keepdims=True) for score in scores]
        )
        powers = [jnp.exp2((score - peak) * scale) for score in scores]
        inverse = 1.0 / sum(jnp.sum(power, 0, keepdims=True) for power in powers)
        mixed = jnp.zeros((HEAD_DIM, rows), F32)
        for step in range(reach + 1):
            prob = (powers[step] * inverse).astype(BF16)
            probs[pl.ds(step * rows, rows), pl.ds(head * rows, rows)] = prob
            mixed = mixed + dot(turned_values[head * groups // heads][step], prob)
        turned[pl.ds(head * HEAD_DIM, HEAD_DIM), :] = mixed.astype(BF16)
        attention[:, pl.ds(head * HEAD_DIM, HEAD_DIM)] = mixed.T.astype(BF16)
        scores = following
    copy.wait()
    in_parts(leads, dot(attention[...], columns_at(local, place, leads[0].shape[1])[...]))


def forward(limits, query, out_proj, blocks, groups, size):
    rows, width = query.shape
    heads = width // HEAD_DIM
    reach = len(blocks) - 1
    share = out_proj.shape[1] // size
    span = (reach + 1) * rows
    outs = pl.pallas_call(
        functools.partial(forward_kernel, reach=reach, groups=groups),
        in_specs=[WHOLE, WHOLE, MAIN] + [WHOLE] * (reach + 1),
        out_specs=[WHOLE] * (4 + PARTS),
        out_shape=[
            pltpu.VMEM((rows, width), BF16),
            pltpu.VMEM((width, rows), BF16),
            pltpu.VMEM((span, heads * rows), BF16),
            pltpu.VMEM(out_proj.shape, BF16),
        ]
        + parts_of(rows, share),
        scratch_shapes=[pltpu.SemaphoreType.DMA],
        compiler_params=PARAMS,
        cost_estimate=estimate(4 * rows * span * width, 8 * rows * span),
        name="forward",
    )(limits, query, main(out_proj), *blocks)
    return outs[:4], outs[4:]


def at_end():
    z = lax.axis_index("head")
    return (z == 0) | (z == lax.axis_size("head") - 1)


def either_kernel(*refs):
    count = (len(refs) - 1) // 2
    ends, inner, outs = refs[:count], refs[count], refs[count + 1 :]
    rows = outs[0].shape[0]
    for index, out in enumerate(outs):

        @pl.when(at_end())
        def _():
            out[...] = ends[index][...]

        @pl.when(jnp.logical_not(at_end()))
        def _():
            out[...] = inner[pl.ds(index * rows, rows), :]


def either(ends, inner):
    rows, width = inner.shape
    count = len(ends)
    return pl.pallas_call(
        either_kernel,
        in_specs=[WHOLE] * (count + 1),
        out_specs=[WHOLE] * count,
        out_shape=[pltpu.VMEM((rows // count, width), BF16)] * count,
        compiler_params=PARAMS,
        cost_estimate=estimate(inner.size, 6 * inner.size),
    )(*ends, inner)


def split_kernel(whole, *parts):
    in_parts(parts, whole[...])


def split(whole):
    return pl.pallas_call(
        split_kernel,
        in_specs=[WHOLE],
        out_specs=[WHOLE] * PARTS,
        out_shape=parts_of(*whole.shape),
        compiler_params=PARAMS,
        cost_estimate=estimate(whole.size, 4 * whole.size),
        name="split",
    )(whole)


def total_kernel(own, *refs):
    parts, out, buffer, sems = refs[:-3], refs[-3], refs[-2], refs[-1]
    rows = parts[0].shape[0]
    copies = []
    for index in range(PARTS):
        spot = pl.ds(index * rows, rows)
        value = own[spot, :].astype(F32)
        for part in parts[index::PARTS]:
            value = value + part[...].astype(F32)
        buffer[spot, :] = value.astype(BF16)
        copies.append(pltpu.make_async_copy(buffer.at[spot], out.at[spot], sems.at[index]))
        copies[-1].start()
    for copy in copies:
        copy.wait()


def total_of(own, *parts):
    return pl.pallas_call(
        total_kernel,
        in_specs=[WHOLE] * (len(parts) + 1),
        out_specs=MAIN,
        out_shape=jax.ShapeDtypeStruct(own.shape, BF16),
        scratch_shapes=[pltpu.VMEM(own.shape, BF16), pltpu.SemaphoreType.DMA((PARTS,))],
        compiler_params=PARAMS,
        cost_estimate=estimate(3 * own.size, 8 * own.size),
        name="total",
    )(own, *parts)


def middle_kernel(attention, own, paired, proj, own_share, partial, *refs):
    far_shares, pair_shares, extra, sem = refs[:PARTS], refs[PARTS:-2], refs[-2], refs[-1]
    size = lax.axis_size("head")
    z = lax.axis_index("head")
    share = extra.shape[1]
    copy = pltpu.make_async_copy(own, extra, sem)
    copy.start()
    block = columns_at(proj, lax.rem(z + size // 2, size), share)
    in_parts(far_shares, dot(attention[...], block[...]))
    block = columns_at(proj, z + 1 - 2 * lax.rem(z, 2), share)
    in_parts(pair_shares, dot(attention[...], block[...]))
    total = dot(block[...], paired[...], NT)
    block = columns_at(proj, z, share)
    own_share[...] = dot(attention[...], block[...]).astype(BF16)
    copy.wait()
    partial[...] = total + dot(block[...], extra[...], NT)


def middle(attention, own, paired, out_proj):
    rows, width = attention.shape
    share = own.shape[1]
    outs = pl.pallas_call(
        middle_kernel,
        in_specs=[WHOLE, MAIN, WHOLE, WHOLE],
        out_specs=[WHOLE] * (2 + 2 * PARTS),
        out_shape=[pltpu.VMEM(own.shape, BF16), pltpu.VMEM((width, rows), F32)]
        + parts_of(rows, share) * 2,
        scratch_shapes=[pltpu.VMEM(own.shape, BF16), pltpu.SemaphoreType.DMA],
        compiler_params=PARAMS,
        cost_estimate=estimate(10 * own.size * width, 8 * own.size),
        name="middle",
    )(attention, main(own), paired, out_proj)
    return outs[0], outs[1], outs[2 : 2 + PARTS], outs[2 + PARTS :]


def add_term(target, partial, block, sources):
    rows = sources[0].shape[0]
    for index, source in enumerate(sources):
        spot = pl.ds(index * rows, rows)
        target[:, spot] = (partial[:, spot] + dot(block[...], source[...], NT)).astype(target.dtype)


def far_kernel(partial, proj, out, *, sources):
    size = lax.axis_size("head")
    z = lax.axis_index("head")
    ends, inner = sources[:PARTS], sources[PARTS:]
    block = columns_at(proj, lax.rem(z + size // 2, size), ends[0].shape[1])

    @pl.when(at_end())
    def _():
        add_term(out, partial, block, ends)

    @pl.when(jnp.logical_not(at_end()))
    def _():
        add_term(out, partial, block, inner)


def far(partial, ends, inner, out_proj):
    width, rows = partial.shape
    return pl.pallas_call(
        lambda partial, proj, *refs: far_kernel(partial, proj, refs[-1], sources=refs[:-1]),
        in_specs=[WHOLE] * (2 + 2 * PARTS),
        out_specs=WHOLE,
        out_shape=pltpu.VMEM((width, rows), F32),
        compiler_params=PARAMS,
        cost_estimate=estimate(2 * rows * width * ends[0].shape[1], 8 * rows * width),
        name="far",
    )(partial, out_proj, *ends, *inner)


def backward_kernel(partial, inner, query, turned, probs, proj, *refs, reach, groups):
    ends, refs = refs[:PARTS], refs[PARTS:]
    blocks = refs[: reach + 1]
    grads = refs[reach + 1 : 2 * reach + 1]
    scores, ups, upstream = refs[2 * reach + 1 :]
    rows, width = query.shape
    heads = width // HEAD_DIM
    ratio = heads // groups
    place = lax.axis_size("head") - 1 - lax.axis_index("head")
    scale = HEAD_DIM ** (-0.5)
    block = columns_at(proj, place, inner.shape[1])

    @pl.when(at_end())
    def _():
        add_term(upstream, partial, block, ends)

    @pl.when(jnp.logical_not(at_end()))
    def _():
        add_term(upstream, partial, block, [inner])

    for head in range(heads):
        up = upstream[pl.ds(head * HEAD_DIM, HEAD_DIM), :]
        ups[pl.ds(head * rows, rows), :] = up.T
        wide = up.astype(F32) * turned[pl.ds(head * HEAD_DIM, HEAD_DIM), :].astype(F32)
        delta = jnp.sum(wide, 0, keepdims=True)
        columns = pl.ds(head * rows, rows)
        for step in range(reach + 1):
            spot = pl.ds(step * rows, rows)
            grad_prob = dot(head_of(blocks[step], groups + head // ratio), up)
            scores[spot, columns] = (
                probs[spot, columns].astype(F32) * (grad_prob - delta)
            ).astype(BF16)
    for group in range(groups):
        tall_query = jnp.concatenate(
            [head_of(query, head) for head in range(group * ratio, (group + 1) * ratio)], 0
        )
        columns = pl.ds(group * ratio * rows, ratio * rows)
        for step in range(1, reach + 1):
            spot = pl.ds(step * rows, rows)
            grads[step - 1][:, pl.ds(group * HEAD_DIM, HEAD_DIM)] = (
                dot(scores[spot, columns], tall_query) * scale
            ).astype(BF16)
            grads[step - 1][:, pl.ds((groups + group) * HEAD_DIM, HEAD_DIM)] = dot(
                probs[spot, columns], ups[columns, :]
            ).astype(BF16)


def backward(partial, ends, inner, query, turned, probs, out_proj, blocks, groups):
    rows, width = query.shape
    heads = width // HEAD_DIM
    reach = len(blocks) - 1
    span = (reach + 1) * rows
    outs = pl.pallas_call(
        functools.partial(backward_kernel, reach=reach, groups=groups),
        in_specs=[WHOLE] * (reach + 7 + PARTS),
        out_specs=[WHOLE] * (reach + 2),
        out_shape=[pltpu.VMEM((rows, 2 * groups * HEAD_DIM), BF16)] * reach
        + [
            pltpu.VMEM(probs.shape, BF16),
            pltpu.VMEM((heads * rows, HEAD_DIM), BF16),
        ],
        scratch_shapes=[pltpu.VMEM((width, rows), BF16)],
        compiler_params=PARAMS,
        cost_estimate=estimate(8 * rows * span * width, 8 * rows * span),
        name="backward",
    )(partial, inner, query, turned, probs, out_proj, *ends, *blocks)
    return outs[:reach], outs[reach], outs[reach + 1]


def finish_kernel(scores, ups, query, probs, *refs, reach, groups):
    blocks = refs[: reach + 1]
    grad_query, grad = refs[reach + 1 :]
    rows, width = query.shape
    heads = width // HEAD_DIM
    ratio = heads // groups
    scale = HEAD_DIM ** (-0.5)
    spot = pl.ds(0, rows)
    for group in range(groups):
        picked = range(group * ratio, (group + 1) * ratio)
        tall_query = jnp.concatenate([head_of(query, head) for head in picked], 0)
        columns = pl.ds(group * ratio * rows, ratio * rows)
        grad[:, pl.ds(group * HEAD_DIM, HEAD_DIM)] = dot(scores[spot, columns], tall_query) * scale
        grad[:, pl.ds((groups + group) * HEAD_DIM, HEAD_DIM)] = dot(
            probs[spot, columns], ups[columns, :]
        )
        keys = jnp.concatenate([head_of(blocks[step], group) for step in range(reach + 1)], 0).T
        for head in picked:
            total = dot(keys, scores[:, pl.ds(head * rows, rows)])
            grad_query[:, pl.ds(head * HEAD_DIM, HEAD_DIM)] = (total * scale).T.astype(BF16)


def finish(scores, ups, query, probs, blocks, groups):
    rows, width = query.shape
    reach = len(blocks) - 1
    span = (reach + 1) * rows
    return pl.pallas_call(
        functools.partial(finish_kernel, reach=reach, groups=groups),
        in_specs=[WHOLE] * (reach + 5),
        out_specs=[WHOLE] * 2,
        out_shape=[
            jax.ShapeDtypeStruct((rows, width), BF16),
            pltpu.VMEM((rows, 2 * groups * HEAD_DIM), F32),
        ],
        compiler_params=PARAMS,
        cost_estimate=estimate(2 * rows * span * width, 4 * rows * span),
        name="finish",
    )(scores, ups, query, probs, *blocks)


def body(queries, key_vectors, values, out_proj, grad_out, windows, slab_order):
    groups = key_vectors.shape[1] // HEAD_DIM
    devices = lax.axis_size("seq")
    size = lax.axis_size("head")
    assert size == 4 and devices % 4 == 0
    reach = min(8, devices // 2)
    half = reach // 2
    even = lax.axis_index("seq") % 2 == 0
    nothing = jnp.zeros((), BF16)

    def outer(array):
        return lax.ppermute(array, "head", [(i ^ 1, i) for i in range(size)])

    def inner(array):
        return lax.ppermute(array, "head", [(1, 2), (2, 1)])

    def shifted(array, step):
        pairs = [((i - step) % devices, i) for i in range(devices)]
        return lax.ppermute(array, "seq", pairs)

    def swapped(array):
        return lax.ppermute(array, "seq", [(i ^ 1, i) for i in range(devices)])

    pair, query, limits = stage(key_vectors, values, queries, windows, slab_order, reach)
    fetched = [pair] + [shifted(pair, 2 * step) for step in range(1, half + 1)]
    traded = [swapped(jnp.where(even, pair, fetched[half]))]
    traded += [swapped(fetched[step]) for step in range(1, half)]
    blocks = [pair]
    for step in range(half):
        blocks.append(jnp.where(even, traded[(step + 1) % half], traded[step]))
        blocks.append(fetched[step + 1])

    both = range(PARTS)
    outer1, inner1 = outer(grad_out), inner(grad_out)
    (attention, turned, probs, proj), lead = forward(
        limits, query, out_proj, blocks, groups, size
    )
    split1 = split(outer1)
    inner2 = [inner(split1[i]) for i in both]
    send2 = either(lead, inner1)
    outer2 = [outer(send2[i]) for i in both]
    own_share, partial, far_share, pair_share = middle(attention, grad_out, outer1, proj)
    send3 = [either([far_share[i]], inner2[i])[0] for i in both]
    outer3 = [outer(send3[i]) for i in both]
    inner3 = [inner(far_share[i] + outer2[i]) for i in both]
    partial = far(partial, outer2, inner2, proj)
    sent, scores, ups = backward(
        partial, outer3, inner1, query, turned, probs, proj, blocks, groups
    )
    inner4 = [inner(lead[i] + outer3[i]) for i in both]
    outer4 = [outer(pair_share[i] + inner3[i]) for i in both]

    taken = [swapped(sent[2 * step]) for step in range(half)]
    total = []
    for step in range(half):
        near = taken[step]
        if step + 1 < half:
            near = jnp.where(even, taken[step + 1], near)
        else:
            near = jnp.where(even, nothing, near)
        total.append(shifted(sent[2 * step + 1] + near, -2 * (step + 1)))
    grad_queries, own = finish(scores, ups, query, probs, blocks, groups)
    own = own + jnp.where(even, taken[0], nothing).astype(F32)
    for part in total:
        own = own + part.astype(F32)
    grad_keys = own[:, : groups * HEAD_DIM].astype(BF16)
    grad_values = own[:, groups * HEAD_DIM :].astype(BF16)
    layer_out = total_of(own_share, *outer4, *inner4)
    return layer_out, grad_queries, grad_keys, grad_values


def solution(mesh):
    in_specs = (
        P("seq", "head"),
        P("seq", "head"),
        P("seq", "head"),
        P("head", None),
        P("seq", "head"),
        P("head"),
        P(),
    )
    out_specs = (P("seq", "head"), P("seq", "head"), P("seq", "head"), P("seq", "head"))
    return jax.shard_map(body, mesh=mesh, in_specs=in_specs, out_specs=out_specs, check_vma=False)
```

```python
import functools

import jax
import jax.numpy as jnp
from jax import lax
from jax.experimental import pallas as pl
from jax.experimental.pallas import tpu as pltpu
from jax.sharding import PartitionSpec as P


HEAD_DIM = 128
LOWEST = -1e30
LOG2_E = 1.4426950408889634
F32 = jnp.float32
BF16 = jnp.bfloat16

NT = (((1,), (1,)), ((), ()))
NN = (((1,), (0,)), ((), ()))

WHOLE = pl.BlockSpec(memory_space=pltpu.VMEM)
MAIN = pl.BlockSpec(memory_space=pltpu.HBM)
PARAMS = pltpu.CompilerParams(vmem_limit_bytes=24 * 1024 * 1024)


def dot(a, b, dims=NN):
    return lax.dot_general(a, b, dims, preferred_element_type=F32)


def head_of(array, index):
    return array[:, index * HEAD_DIM : (index + 1) * HEAD_DIM]


def columns_at(proj, index, share):
    return proj.at[:, pl.ds(pl.multiple_of(index * share, share), share)]


PARTS = 2


def parts_of(rows, width):
    return [pltpu.VMEM((rows // PARTS, width), BF16)] * PARTS


def in_parts(refs, whole):
    rows = refs[0].shape[0]
    for index, ref in enumerate(refs):
        ref[...] = whole[index * rows : (index + 1) * rows].astype(BF16)


def main(array):
    return pltpu.with_memory_space_constraint(array, pltpu.HBM)


def estimate(flops, size):
    return pl.CostEstimate(flops=flops, bytes_accessed=size, transcendentals=0)


def stage_kernel(keys, values, queries, windows, order, pair, query, limits, spans, slabs, sems, *, reach):
    rows, width = keys.shape
    copies = [
        pltpu.make_async_copy(windows, spans, sems.at[0]),
        pltpu.make_async_copy(order, slabs, sems.at[1]),
        pltpu.make_async_copy(keys, pair.at[:, pl.ds(0, width)], sems.at[2]),
        pltpu.make_async_copy(values, pair.at[:, pl.ds(width, width)], sems.at[3]),
        pltpu.make_async_copy(queries, query, sems.at[4]),
    ]
    for copy in copies:
        copy.start()
    copies[0].wait()
    copies[1].wait()
    slab = slabs[lax.axis_index("seq")]
    for head in range(windows.shape[0]):
        for step in range(reach + 1):
            limit = jnp.where(slab >= step, spans[head] - step * rows, -rows)
            limits[pl.ds(head * (reach + 1) + step, 1), :] = jnp.full((1, rows), limit, jnp.int32)
    for copy in copies[2:]:
        copy.wait()


def stage(key_vectors, values, queries, windows, slab_order, reach):
    rows, width = key_vectors.shape
    heads = windows.shape[0]
    return pl.pallas_call(
        functools.partial(stage_kernel, reach=reach),
        in_specs=[MAIN] * 5,
        out_specs=[WHOLE] * 3,
        out_shape=[
            pltpu.VMEM((rows, 2 * width), BF16),
            pltpu.VMEM(queries.shape, BF16),
            pltpu.VMEM((heads * (reach + 1), rows), jnp.int32),
        ],
        scratch_shapes=[
            pltpu.SMEM(windows.shape, jnp.int32),
            pltpu.SMEM(slab_order.shape, jnp.int32),
            pltpu.SemaphoreType.DMA((5,)),
        ],
        compiler_params=PARAMS,
        cost_estimate=estimate(rows * width, 8 * rows * width),
        name="stage",
    )(*[main(array) for array in (key_vectors, values, queries, windows, slab_order)])


def forward_kernel(limits, query, proj, *refs, reach, groups):
    blocks = refs[: reach + 1]
    attention, turned, probs, local = refs[reach + 1 : reach + 5]
    leads, sem = refs[reach + 5 : -1], refs[-1]
    rows, width = query.shape
    heads = width // HEAD_DIM
    size = lax.axis_size("head")
    place = size - 1 - lax.axis_index("head")
    copy = pltpu.make_async_copy(proj, local, sem)
    copy.start()
    scale = HEAD_DIM ** (-0.5) * LOG2_E
    offset = lax.broadcasted_iota(jnp.int32, (rows, rows), 1) - lax.broadcasted_iota(
        jnp.int32, (rows, rows), 0
    )
    turned_values = [
        [head_of(blocks[step], groups + group).T for step in range(reach + 1)]
        for group in range(groups)
    ]

    def head_scores(head):
        scores = []
        for step in range(reach + 1):
            score = dot(head_of(blocks[step], head * groups // heads), head_of(query, head), NT)
            mask = offset < limits[pl.ds(head * (reach + 1) + step, 1), :]
            if step == 0:
                mask = mask & (offset >= 0)
            scores.append(jnp.where(mask, score, LOWEST))
        return scores

    scores = head_scores(0)
    for head in range(heads):
        following = head_scores(head + 1) if head + 1 < heads else None
        peak = functools.reduce(
            jnp.maximum, [jnp.max(score, 0, keepdims=True) for score in scores]
        )
        powers = [jnp.exp2((score - peak) * scale) for score in scores]
        inverse = 1.0 / sum(jnp.sum(power, 0, keepdims=True) for power in powers)
        mixed = jnp.zeros((HEAD_DIM, rows), F32)
        for step in range(reach + 1):
            prob = (powers[step] * inverse).astype(BF16)
            probs[pl.ds(step * rows, rows), pl.ds(head * rows, rows)] = prob
            mixed = mixed + dot(turned_values[head * groups // heads][step], prob)
        turned[pl.ds(head * HEAD_DIM, HEAD_DIM), :] = mixed.astype(BF16)
        attention[:, pl.ds(head * HEAD_DIM, HEAD_DIM)] = mixed.T.astype(BF16)
        scores = following
    copy.wait()
    in_parts(leads, dot(attention[...], columns_at(local, place, leads[0].shape[1])[...]))


def forward(limits, query, out_proj, blocks, groups, size):
    rows, width = query.shape
    heads = width // HEAD_DIM
    reach = len(blocks) - 1
    share = out_proj.shape[1] // size
    span = (reach + 1) * rows
    outs = pl.pallas_call(
        functools.partial(forward_kernel, reach=reach, groups=groups),
        in_specs=[WHOLE, WHOLE, MAIN] + [WHOLE] * (reach + 1),
        out_specs=[WHOLE] * (4 + PARTS),
        out_shape=[
            pltpu.VMEM((rows, width), BF16),
            pltpu.VMEM((width, rows), BF16),
            pltpu.VMEM((span, heads * rows), BF16),
            pltpu.VMEM(out_proj.shape, BF16),
        ]
        + parts_of(rows, share),
        scratch_shapes=[pltpu.SemaphoreType.DMA],
        compiler_params=PARAMS,
        cost_estimate=estimate(4 * rows * span * width, 8 * rows * span),
        name="forward",
    )(limits, query, main(out_proj), *blocks)
    return outs[:4], outs[4:]


def at_end():
    z = lax.axis_index("head")
    return (z == 0) | (z == lax.axis_size("head") - 1)


def either_kernel(*refs):
    count = (len(refs) - 1) // 2
    ends, inner, outs = refs[:count], refs[count], refs[count + 1 :]
    rows = outs[0].shape[0]
    for index, out in enumerate(outs):

        @pl.when(at_end())
        def _():
            out[...] = ends[index][...]

        @pl.when(jnp.logical_not(at_end()))
        def _():
            out[...] = inner[pl.ds(index * rows, rows), :]


def either(ends, inner):
    rows, width = inner.shape
    count = len(ends)
    return pl.pallas_call(
        either_kernel,
        in_specs=[WHOLE] * (count + 1),
        out_specs=[WHOLE] * count,
        out_shape=[pltpu.VMEM((rows // count, width), BF16)] * count,
        compiler_params=PARAMS,
        cost_estimate=estimate(inner.size, 6 * inner.size),
    )(*ends, inner)


def carry_kernel(share, passed, out):
    @pl.when(at_end())
    def _():
        out[...] = share[...]

    @pl.when(jnp.logical_not(at_end()))
    def _():
        out[...] = share[...] + passed[...]


def carry(share, passed):
    return pl.pallas_call(
        carry_kernel,
        in_specs=[WHOLE] * 2,
        out_specs=WHOLE,
        out_shape=pltpu.VMEM(share.shape, BF16),
        compiler_params=PARAMS,
        cost_estimate=estimate(share.size, 6 * share.size),
    )(share, passed)


def split_kernel(whole, *parts):
    in_parts(parts, whole[...])


def split(whole):
    return pl.pallas_call(
        split_kernel,
        in_specs=[WHOLE],
        out_specs=[WHOLE] * PARTS,
        out_shape=parts_of(*whole.shape),
        compiler_params=PARAMS,
        cost_estimate=estimate(whole.size, 4 * whole.size),
        name="split",
    )(whole)


def total_kernel(own, *refs):
    outer, inner, (out, buffer, sems) = refs[:PARTS], refs[PARTS:-3], refs[-3:]
    rows = outer[0].shape[0]
    copies = []
    for index in range(PARTS):
        spot = pl.ds(index * rows, rows)
        value = own[spot, :].astype(F32) + outer[index][...].astype(F32)

        @pl.when(at_end())
        def _():
            buffer[spot, :] = value.astype(BF16)

        @pl.when(jnp.logical_not(at_end()))
        def _():
            buffer[spot, :] = (value + inner[index][...].astype(F32)).astype(BF16)

        copies.append(pltpu.make_async_copy(buffer.at[spot], out.at[spot], sems.at[index]))
        copies[-1].start()
    for copy in copies:
        copy.wait()


def total_of(own, *parts):
    return pl.pallas_call(
        total_kernel,
        in_specs=[WHOLE] * (len(parts) + 1),
        out_specs=MAIN,
        out_shape=jax.ShapeDtypeStruct(own.shape, BF16),
        scratch_shapes=[pltpu.VMEM(own.shape, BF16), pltpu.SemaphoreType.DMA((PARTS,))],
        compiler_params=PARAMS,
        cost_estimate=estimate(3 * own.size, 8 * own.size),
        name="total",
    )(own, *parts)


def middle_kernel(attention, own, paired, proj, own_share, partial, *refs):
    far_shares, pair_shares, extra, sem = refs[:PARTS], refs[PARTS:-2], refs[-2], refs[-1]
    size = lax.axis_size("head")
    z = lax.axis_index("head")
    share = extra.shape[1]
    copy = pltpu.make_async_copy(own, extra, sem)
    copy.start()
    block = columns_at(proj, lax.rem(z + size // 2, size), share)
    in_parts(far_shares, dot(attention[...], block[...]))
    block = columns_at(proj, z + 1 - 2 * lax.rem(z, 2), share)
    in_parts(pair_shares, dot(attention[...], block[...]))
    total = dot(block[...], paired[...], NT)
    block = columns_at(proj, z, share)
    own_share[...] = dot(attention[...], block[...]).astype(BF16)
    copy.wait()
    partial[...] = total + dot(block[...], extra[...], NT)


def middle(attention, own, paired, out_proj):
    rows, width = attention.shape
    share = own.shape[1]
    outs = pl.pallas_call(
        middle_kernel,
        in_specs=[WHOLE, MAIN, WHOLE, WHOLE],
        out_specs=[WHOLE] * (2 + 2 * PARTS),
        out_shape=[pltpu.VMEM(own.shape, BF16), pltpu.VMEM((width, rows), F32)]
        + parts_of(rows, share) * 2,
        scratch_shapes=[pltpu.VMEM(own.shape, BF16), pltpu.SemaphoreType.DMA],
        compiler_params=PARAMS,
        cost_estimate=estimate(10 * own.size * width, 8 * own.size),
        name="middle",
    )(attention, main(own), paired, out_proj)
    return outs[0], outs[1], outs[2 : 2 + PARTS], outs[2 + PARTS :]


def add_term(target, partial, block, sources):
    rows = sources[0].shape[0]
    for index, source in enumerate(sources):
        spot = pl.ds(index * rows, rows)
        target[:, spot] = (partial[:, spot] + dot(block[...], source[...], NT)).astype(target.dtype)


def far_kernel(partial, proj, out, *, sources):
    size = lax.axis_size("head")
    z = lax.axis_index("head")
    ends, inner = sources[:PARTS], sources[PARTS:]
    block = columns_at(proj, lax.rem(z + size // 2, size), ends[0].shape[1])

    @pl.when(at_end())
    def _():
        add_term(out, partial, block, ends)

    @pl.when(jnp.logical_not(at_end()))
    def _():
        add_term(out, partial, block, inner)


def far(partial, ends, inner, out_proj):
    width, rows = partial.shape
    return pl.pallas_call(
        lambda partial, proj, *refs: far_kernel(partial, proj, refs[-1], sources=refs[:-1]),
        in_specs=[WHOLE] * (2 + 2 * PARTS),
        out_specs=WHOLE,
        out_shape=pltpu.VMEM((width, rows), F32),
        compiler_params=PARAMS,
        cost_estimate=estimate(2 * rows * width * ends[0].shape[1], 8 * rows * width),
        name="far",
    )(partial, out_proj, *ends, *inner)


def backward_kernel(partial, inner, query, turned, probs, proj, *refs, reach, groups):
    ends, refs = refs[:PARTS], refs[PARTS:]
    blocks = refs[: reach + 1]
    grads = refs[reach + 1 : 2 * reach + 1]
    scores, ups, upstream = refs[2 * reach + 1 :]
    rows, width = query.shape
    heads = width // HEAD_DIM
    ratio = heads // groups
    place = lax.axis_size("head") - 1 - lax.axis_index("head")
    scale = HEAD_DIM ** (-0.5)
    block = columns_at(proj, place, inner.shape[1])

    @pl.when(at_end())
    def _():
        add_term(upstream, partial, block, ends)

    @pl.when(jnp.logical_not(at_end()))
    def _():
        add_term(upstream, partial, block, [inner])

    for head in range(heads):
        up = upstream[pl.ds(head * HEAD_DIM, HEAD_DIM), :]
        ups[pl.ds(head * rows, rows), :] = up.T
        wide = up.astype(F32) * turned[pl.ds(head * HEAD_DIM, HEAD_DIM), :].astype(F32)
        delta = jnp.sum(wide, 0, keepdims=True)
        columns = pl.ds(head * rows, rows)
        for step in range(reach + 1):
            spot = pl.ds(step * rows, rows)
            grad_prob = dot(head_of(blocks[step], groups + head // ratio), up)
            scores[spot, columns] = (
                probs[spot, columns].astype(F32) * (grad_prob - delta)
            ).astype(BF16)
    for group in range(groups):
        tall_query = jnp.concatenate(
            [head_of(query, head) for head in range(group * ratio, (group + 1) * ratio)], 0
        )
        columns = pl.ds(group * ratio * rows, ratio * rows)
        for step in range(1, reach + 1):
            spot = pl.ds(step * rows, rows)
            grads[step - 1][:, pl.ds(group * HEAD_DIM, HEAD_DIM)] = (
                dot(scores[spot, columns], tall_query) * scale
            ).astype(BF16)
            grads[step - 1][:, pl.ds((groups + group) * HEAD_DIM, HEAD_DIM)] = dot(
                probs[spot, columns], ups[columns, :]
            ).astype(BF16)


def backward(partial, ends, inner, query, turned, probs, out_proj, blocks, groups):
    rows, width = query.shape
    heads = width // HEAD_DIM
    reach = len(blocks) - 1
    span = (reach + 1) * rows
    outs = pl.pallas_call(
        functools.partial(backward_kernel, reach=reach, groups=groups),
        in_specs=[WHOLE] * (reach + 7 + PARTS),
        out_specs=[WHOLE] * (reach + 2),
        out_shape=[pltpu.VMEM((rows, 2 * groups * HEAD_DIM), BF16)] * reach
        + [
            pltpu.VMEM(probs.shape, BF16),
            pltpu.VMEM((heads * rows, HEAD_DIM), BF16),
        ],
        scratch_shapes=[pltpu.VMEM((width, rows), BF16)],
        compiler_params=PARAMS,
        cost_estimate=estimate(8 * rows * span * width, 8 * rows * span),
        name="backward",
    )(partial, inner, query, turned, probs, out_proj, *ends, *blocks)
    return outs[:reach], outs[reach], outs[reach + 1]


def finish_kernel(scores, ups, query, probs, *refs, reach, groups):
    blocks = refs[: reach + 1]
    grad_query, grad = refs[reach + 1 :]
    rows, width = query.shape
    heads = width // HEAD_DIM
    ratio = heads // groups
    scale = HEAD_DIM ** (-0.5)
    spot = pl.ds(0, rows)
    for group in range(groups):
        picked = range(group * ratio, (group + 1) * ratio)
        tall_query = jnp.concatenate([head_of(query, head) for head in picked], 0)
        columns = pl.ds(group * ratio * rows, ratio * rows)
        grad[:, pl.ds(group * HEAD_DIM, HEAD_DIM)] = dot(scores[spot, columns], tall_query) * scale
        grad[:, pl.ds((groups + group) * HEAD_DIM, HEAD_DIM)] = dot(
            probs[spot, columns], ups[columns, :]
        )
        keys = jnp.concatenate([head_of(blocks[step], group) for step in range(reach + 1)], 0).T
        for head in picked:
            total = dot(keys, scores[:, pl.ds(head * rows, rows)])
            grad_query[:, pl.ds(head * HEAD_DIM, HEAD_DIM)] = (total * scale).T.astype(BF16)


def finish(scores, ups, query, probs, blocks, groups):
    rows, width = query.shape
    reach = len(blocks) - 1
    span = (reach + 1) * rows
    return pl.pallas_call(
        functools.partial(finish_kernel, reach=reach, groups=groups),
        in_specs=[WHOLE] * (reach + 5),
        out_specs=[WHOLE] * 2,
        out_shape=[
            jax.ShapeDtypeStruct((rows, width), BF16),
            pltpu.VMEM((rows, 2 * groups * HEAD_DIM), F32),
        ],
        compiler_params=PARAMS,
        cost_estimate=estimate(2 * rows * span * width, 4 * rows * span),
        name="finish",
    )(scores, ups, query, probs, *blocks)


def body(queries, key_vectors, values, out_proj, grad_out, windows, slab_order):
    groups = key_vectors.shape[1] // HEAD_DIM
    devices = lax.axis_size("seq")
    size = lax.axis_size("head")
    assert size == 4 and devices % 4 == 0
    reach = min(8, devices // 2)
    half = reach // 2
    even = lax.axis_index("seq") % 2 == 0
    nothing = jnp.zeros((), BF16)

    across = []
    for i in range(devices):
        for first, second in ((1, (i, 2)), (2, (i, 1)), (0, (i ^ 1, 0)), (3, (i ^ 1, 3))):
            across.append((i * size + first, second[0] * size + second[1]))

    def outer(array):
        return lax.ppermute(array, "head", [(i ^ 1, i) for i in range(size)])

    def inner(array):
        return lax.ppermute(array, ("seq", "head"), across)

    def shifted(array, step):
        pairs = [((i - step) % devices, i) for i in range(devices)]
        return lax.ppermute(array, "seq", pairs)

    def swapped(array):
        return lax.ppermute(array, "seq", [(i ^ 1, i) for i in range(devices)])

    pair, query, limits = stage(key_vectors, values, queries, windows, slab_order, reach)
    fetched = [pair] + [shifted(pair, 2 * step) for step in range(1, half + 1)]
    traded = [swapped(jnp.where(even, pair, fetched[half]))]
    traded += [swapped(fetched[step]) for step in range(1, half)]
    blocks = [pair]
    for step in range(half):
        blocks.append(jnp.where(even, traded[(step + 1) % half], traded[step]))
        blocks.append(fetched[step + 1])

    both = range(PARTS)
    outer1, inner1 = outer(grad_out), inner(grad_out)
    (attention, turned, probs, proj), lead = forward(
        limits, query, out_proj, blocks, groups, size
    )
    split1 = split(outer1)
    inner2 = [inner(split1[i]) for i in both]
    send2 = either(lead, inner1)
    outer2 = [outer(send2[i]) for i in both]
    own_share, partial, far_share, pair_share = middle(attention, grad_out, outer1, proj)
    send3 = [either([far_share[i]], inner2[i])[0] for i in both]
    outer3 = [outer(send3[i]) for i in both]
    inner3 = [inner(far_share[i] + outer2[i]) for i in both]
    partial = far(partial, outer2, inner2, proj)
    sent, scores, ups = backward(
        partial, outer3, inner1, query, turned, probs, proj, blocks, groups
    )
    inner4 = [inner(lead[i] + outer3[i]) for i in both]
    outer4 = [outer(carry(pair_share[i], inner3[i])) for i in both]

    taken = [swapped(sent[2 * step]) for step in range(half)]
    total = []
    for step in range(half):
        near = taken[step]
        if step + 1 < half:
            near = jnp.where(even, taken[step + 1], near)
        else:
            near = jnp.where(even, nothing, near)
        total.append(shifted(sent[2 * step + 1] + near, -2 * (step + 1)))
    grad_queries, own = finish(scores, ups, query, probs, blocks, groups)
    own = own + jnp.where(even, taken[0], nothing).astype(F32)
    for part in total:
        own = own + part.astype(F32)
    grad_keys = own[:, : groups * HEAD_DIM].astype(BF16)
    grad_values = own[:, groups * HEAD_DIM :].astype(BF16)
    layer_out = total_of(own_share, *outer4, *inner4)
    return layer_out, grad_queries, grad_keys, grad_values


def solution(mesh):
    in_specs = (
        P("seq", "head"),
        P("seq", "head"),
        P("seq", "head"),
        P("head", None),
        P("seq", "head"),
        P("head"),
        P(),
    )
    out_specs = (P("seq", "head"), P("seq", "head"), P("seq", "head"), P("seq", "head"))
    return jax.shard_map(body, mesh=mesh, in_specs=in_specs, out_specs=out_specs, check_vma=False)
```

```python
import functools

import jax
import jax.numpy as jnp
from jax import lax
from jax.experimental import pallas as pl
from jax.experimental.pallas import tpu as pltpu
from jax.sharding import PartitionSpec as P


HEAD_DIM = 128
LOWEST = -1e30
LOG2_E = 1.4426950408889634
F32 = jnp.float32
BF16 = jnp.bfloat16

NT = (((1,), (1,)), ((), ()))
NN = (((1,), (0,)), ((), ()))

WHOLE = pl.BlockSpec(memory_space=pltpu.VMEM)
MAIN = pl.BlockSpec(memory_space=pltpu.HBM)
PARAMS = pltpu.CompilerParams(vmem_limit_bytes=24 * 1024 * 1024)


def dot(a, b, dims=NN):
    return lax.dot_general(a, b, dims, preferred_element_type=F32)


def head_of(array, index):
    return array[:, index * HEAD_DIM : (index + 1) * HEAD_DIM]


def columns_at(proj, index, share):
    return proj.at[:, pl.ds(pl.multiple_of(index * share, share), share)]


PARTS = 2


def parts_of(rows, width):
    return [pltpu.VMEM((rows // PARTS, width), BF16)] * PARTS


def in_parts(refs, whole):
    rows = refs[0].shape[0]
    for index, ref in enumerate(refs):
        ref[...] = whole[index * rows : (index + 1) * rows].astype(BF16)


def main(array):
    return pltpu.with_memory_space_constraint(array, pltpu.HBM)


def estimate(flops, size):
    return pl.CostEstimate(flops=flops, bytes_accessed=size, transcendentals=0)


def stage_kernel(keys, values, queries, windows, order, pair, query, limits, spans, slabs, sems, *, reach):
    rows, width = keys.shape
    copies = [
        pltpu.make_async_copy(windows, spans, sems.at[0]),
        pltpu.make_async_copy(order, slabs, sems.at[1]),
        pltpu.make_async_copy(keys, pair.at[:, pl.ds(0, width)], sems.at[2]),
        pltpu.make_async_copy(values, pair.at[:, pl.ds(width, width)], sems.at[3]),
        pltpu.make_async_copy(queries, query, sems.at[4]),
    ]
    for copy in copies:
        copy.start()
    copies[0].wait()
    copies[1].wait()
    slab = slabs[lax.axis_index("seq")]
    for head in range(windows.shape[0]):
        for step in range(reach + 1):
            limit = jnp.where(slab >= step, spans[head] - step * rows, -rows)
            limits[pl.ds(head * (reach + 1) + step, 1), :] = jnp.full((1, rows), limit, jnp.int32)
    for copy in copies[2:]:
        copy.wait()


def stage(key_vectors, values, queries, windows, slab_order, reach):
    rows, width = key_vectors.shape
    heads = windows.shape[0]
    return pl.pallas_call(
        functools.partial(stage_kernel, reach=reach),
        in_specs=[MAIN] * 5,
        out_specs=[WHOLE] * 3,
        out_shape=[
            pltpu.VMEM((rows, 2 * width), BF16),
            pltpu.VMEM(queries.shape, BF16),
            pltpu.VMEM((heads * (reach + 1), rows), jnp.int32),
        ],
        scratch_shapes=[
            pltpu.SMEM(windows.shape, jnp.int32),
            pltpu.SMEM(slab_order.shape, jnp.int32),
            pltpu.SemaphoreType.DMA((5,)),
        ],
        compiler_params=PARAMS,
        cost_estimate=estimate(rows * width, 8 * rows * width),
        name="stage",
    )(*[main(array) for array in (key_vectors, values, queries, windows, slab_order)])


def bring_kernel(source, out, sem):
    copy = pltpu.make_async_copy(source, out, sem)
    copy.start()
    copy.wait()


def bring(array):
    return pl.pallas_call(
        bring_kernel,
        in_specs=[MAIN],
        out_specs=WHOLE,
        out_shape=pltpu.VMEM(array.shape, array.dtype),
        scratch_shapes=[pltpu.SemaphoreType.DMA],
        compiler_params=PARAMS,
        cost_estimate=estimate(array.size, 4 * array.size),
        name="bring",
    )(main(array))


def forward_kernel(limits, query, proj, *refs, part, reach, groups):
    blocks = refs[: reach + 1]
    attention, turned, probs, lead = refs[reach + 1 : reach + 5]
    keys = blocks[0].shape[0]
    width = query.shape[1]
    rows = attention.shape[0]
    heads = width // HEAD_DIM
    size = lax.axis_size("head")
    place = size - 1 - lax.axis_index("head")
    scale = HEAD_DIM ** (-0.5) * LOG2_E
    offset = (
        lax.broadcasted_iota(jnp.int32, (keys, rows), 1)
        - lax.broadcasted_iota(jnp.int32, (keys, rows), 0)
        + part * rows
    )
    turned_values = [
        [head_of(blocks[step], groups + group).T for step in range(reach + 1)]
        for group in range(groups)
    ]

    def head_scores(head):
        scores = []
        picked = query[pl.ds(part * rows, rows), pl.ds(head * HEAD_DIM, HEAD_DIM)]
        for step in range(reach + 1):
            score = dot(head_of(blocks[step], head * groups // heads), picked, NT)
            mask = offset < limits[pl.ds(head * (reach + 1) + step, 1), pl.ds(0, rows)]
            if step == 0:
                mask = mask & (offset >= 0)
            scores.append(jnp.where(mask, score, LOWEST))
        return scores

    scores = head_scores(0)
    for head in range(heads):
        following = head_scores(head + 1) if head + 1 < heads else None
        peak = functools.reduce(
            jnp.maximum, [jnp.max(score, 0, keepdims=True) for score in scores]
        )
        powers = [jnp.exp2((score - peak) * scale) for score in scores]
        inverse = 1.0 / sum(jnp.sum(power, 0, keepdims=True) for power in powers)
        mixed = jnp.zeros((HEAD_DIM, rows), F32)
        for step in range(reach + 1):
            prob = (powers[step] * inverse).astype(BF16)
            probs[pl.ds(step * keys, keys), pl.ds(head * rows, rows)] = prob
            mixed = mixed + dot(turned_values[head * groups // heads][step], prob)
        turned[pl.ds(head * HEAD_DIM, HEAD_DIM), :] = mixed.astype(BF16)
        attention[:, pl.ds(head * HEAD_DIM, HEAD_DIM)] = mixed.T.astype(BF16)
        scores = following
    lead[...] = dot(attention[...], columns_at(proj, place, lead.shape[1])[...]).astype(BF16)


def forward(limits, query, proj, blocks, part, groups, size):
    rows, width = query.shape
    heads = width // HEAD_DIM
    reach = len(blocks) - 1
    span = (reach + 1) * rows
    rows = rows // PARTS
    return pl.pallas_call(
        functools.partial(forward_kernel, part=part, reach=reach, groups=groups),
        in_specs=[WHOLE] * (reach + 4),
        out_specs=[WHOLE] * 4,
        out_shape=[
            pltpu.VMEM((rows, width), BF16),
            pltpu.VMEM((width, rows), BF16),
            pltpu.VMEM((span, heads * rows), BF16),
            pltpu.VMEM((rows, proj.shape[1] // size), BF16),
        ],
        compiler_params=PARAMS,
        cost_estimate=estimate(4 * rows * span * width, 8 * rows * span),
    )(limits, query, proj, *blocks)


def side_by_side(parts, spot, columns):
    return jnp.concatenate([part[spot, columns] for part in parts], 1)


def at_end():
    z = lax.axis_index("head")
    return (z == 0) | (z == lax.axis_size("head") - 1)


def either_kernel(ends, inner, out, *, first):
    @pl.when(at_end())
    def _():
        out[...] = ends[...]

    @pl.when(jnp.logical_not(at_end()))
    def _():
        out[...] = inner[pl.ds(first, out.shape[0]), :]


def either(ends, inner, first):
    return pl.pallas_call(
        functools.partial(either_kernel, first=first),
        in_specs=[WHOLE] * 2,
        out_specs=WHOLE,
        out_shape=pltpu.VMEM(ends.shape, BF16),
        compiler_params=PARAMS,
        cost_estimate=estimate(ends.size, 6 * ends.size),
    )(ends, inner)


def carry_kernel(share, passed, out):
    @pl.when(at_end())
    def _():
        out[...] = share[...]

    @pl.when(jnp.logical_not(at_end()))
    def _():
        out[...] = share[...] + passed[...]


def carry(share, passed):
    return pl.pallas_call(
        carry_kernel,
        in_specs=[WHOLE] * 2,
        out_specs=WHOLE,
        out_shape=pltpu.VMEM(share.shape, BF16),
        compiler_params=PARAMS,
        cost_estimate=estimate(share.size, 6 * share.size),
    )(share, passed)


def split_kernel(whole, *parts):
    in_parts(parts, whole[...])


def split(whole):
    return pl.pallas_call(
        split_kernel,
        in_specs=[WHOLE],
        out_specs=[WHOLE] * PARTS,
        out_shape=parts_of(*whole.shape),
        compiler_params=PARAMS,
        cost_estimate=estimate(whole.size, 4 * whole.size),
        name="split",
    )(whole)


def total_kernel(own, *refs):
    outer, inner, (out, buffer, sems) = refs[:PARTS], refs[PARTS:-3], refs[-3:]
    rows = outer[0].shape[0]
    copies = []
    for index in range(PARTS):
        spot = pl.ds(index * rows, rows)
        value = own[spot, :].astype(F32) + outer[index][...].astype(F32)

        @pl.when(at_end())
        def _():
            buffer[spot, :] = value.astype(BF16)

        @pl.when(jnp.logical_not(at_end()))
        def _():
            buffer[spot, :] = (value + inner[index][...].astype(F32)).astype(BF16)

        copies.append(pltpu.make_async_copy(buffer.at[spot], out.at[spot], sems.at[index]))
        copies[-1].start()
    for copy in copies:
        copy.wait()


def total_of(own, *parts):
    return pl.pallas_call(
        total_kernel,
        in_specs=[WHOLE] * (len(parts) + 1),
        out_specs=MAIN,
        out_shape=jax.ShapeDtypeStruct(own.shape, BF16),
        scratch_shapes=[pltpu.VMEM(own.shape, BF16), pltpu.SemaphoreType.DMA((PARTS,))],
        compiler_params=PARAMS,
        cost_estimate=estimate(3 * own.size, 8 * own.size),
        name="total",
    )(own, *parts)


def middle_kernel(own, paired, proj, *refs):
    attention = jnp.concatenate([part[...] for part in refs[:PARTS]], 0)
    own_share, partial = refs[PARTS : PARTS + 2]
    far_shares, pair_shares = refs[PARTS + 2 : 2 * PARTS + 2], refs[2 * PARTS + 2 : -2]
    extra, sem = refs[-2:]
    size = lax.axis_size("head")
    z = lax.axis_index("head")
    share = extra.shape[1]
    copy = pltpu.make_async_copy(own, extra, sem)
    copy.start()
    block = columns_at(proj, lax.rem(z + size // 2, size), share)
    in_parts(far_shares, dot(attention, block[...]))
    block = columns_at(proj, z + 1 - 2 * lax.rem(z, 2), share)
    in_parts(pair_shares, dot(attention, block[...]))
    total = dot(block[...], paired[...], NT)
    block = columns_at(proj, z, share)
    own_share[...] = dot(attention, block[...]).astype(BF16)
    copy.wait()
    partial[...] = total + dot(block[...], extra[...], NT)


def middle(attention, own, paired, out_proj):
    rows, share = own.shape
    width = attention[0].shape[1]
    outs = pl.pallas_call(
        middle_kernel,
        in_specs=[MAIN, WHOLE, WHOLE] + [WHOLE] * PARTS,
        out_specs=[WHOLE] * (2 + 2 * PARTS),
        out_shape=[pltpu.VMEM(own.shape, BF16), pltpu.VMEM((width, rows), F32)]
        + parts_of(rows, share) * 2,
        scratch_shapes=[pltpu.VMEM(own.shape, BF16), pltpu.SemaphoreType.DMA],
        compiler_params=PARAMS,
        cost_estimate=estimate(10 * own.size * width, 8 * own.size),
        name="middle",
    )(main(own), paired, out_proj, *attention)
    return outs[0], outs[1], outs[2 : 2 + PARTS], outs[2 + PARTS :]


def add_term(target, partial, block, sources):
    rows = sources[0].shape[0]
    for index, source in enumerate(sources):
        spot = pl.ds(index * rows, rows)
        target[:, spot] = (partial[:, spot] + dot(block[...], source[...], NT)).astype(target.dtype)


def far_kernel(partial, proj, out, *, sources):
    size = lax.axis_size("head")
    z = lax.axis_index("head")
    ends, inner = sources[:PARTS], sources[PARTS:]
    block = columns_at(proj, lax.rem(z + size // 2, size), ends[0].shape[1])

    @pl.when(at_end())
    def _():
        add_term(out, partial, block, ends)

    @pl.when(jnp.logical_not(at_end()))
    def _():
        add_term(out, partial, block, inner)


def far(partial, ends, inner, out_proj):
    width, rows = partial.shape
    return pl.pallas_call(
        lambda partial, proj, *refs: far_kernel(partial, proj, refs[-1], sources=refs[:-1]),
        in_specs=[WHOLE] * (2 + 2 * PARTS),
        out_specs=WHOLE,
        out_shape=pltpu.VMEM((width, rows), F32),
        compiler_params=PARAMS,
        cost_estimate=estimate(2 * rows * width * ends[0].shape[1], 8 * rows * width),
        name="far",
    )(partial, out_proj, *ends, *inner)


def value_grad(probs, spot, ups, group, ratio, rows):
    picked = range(group * ratio, (group + 1) * ratio)
    part = rows // PARTS
    wide = jnp.concatenate(
        [side_by_side(probs, spot, pl.ds(head * part, part)) for head in picked], 1
    )
    return dot(wide, ups[pl.ds(group * ratio * rows, ratio * rows), :])


def backward_kernel(partial, inner, query, proj, *refs, reach, groups):
    turned, probs, refs = refs[:PARTS], refs[PARTS : 2 * PARTS], refs[2 * PARTS :]
    ends, refs = refs[:PARTS], refs[PARTS:]
    blocks = refs[: reach + 1]
    grads = refs[reach + 1 : 2 * reach + 1]
    scores, ups, upstream = refs[2 * reach + 1 :]
    rows, width = query.shape
    heads = width // HEAD_DIM
    ratio = heads // groups
    place = lax.axis_size("head") - 1 - lax.axis_index("head")
    scale = HEAD_DIM ** (-0.5)
    block = columns_at(proj, place, inner.shape[1])

    @pl.when(at_end())
    def _():
        add_term(upstream, partial, block, ends)

    @pl.when(jnp.logical_not(at_end()))
    def _():
        add_term(upstream, partial, block, [inner])

    for head in range(heads):
        up = upstream[pl.ds(head * HEAD_DIM, HEAD_DIM), :]
        ups[pl.ds(head * rows, rows), :] = up.T
        mixed = side_by_side(turned, pl.ds(head * HEAD_DIM, HEAD_DIM), slice(None))
        wide = up.astype(F32) * mixed.astype(F32)
        delta = jnp.sum(wide, 0, keepdims=True)
        columns = pl.ds(head * rows, rows)
        for step in range(reach + 1):
            spot = pl.ds(step * rows, rows)
            grad_prob = dot(head_of(blocks[step], groups + head // ratio), up)
            prob = side_by_side(probs, spot, pl.ds(head * rows // PARTS, rows // PARTS))
            scores[spot, columns] = (prob.astype(F32) * (grad_prob - delta)).astype(BF16)
    for group in range(groups):
        tall_query = jnp.concatenate(
            [head_of(query, head) for head in range(group * ratio, (group + 1) * ratio)], 0
        )
        columns = pl.ds(group * ratio * rows, ratio * rows)
        for step in range(1, reach + 1):
            spot = pl.ds(step * rows, rows)
            grads[step - 1][:, pl.ds(group * HEAD_DIM, HEAD_DIM)] = (
                dot(scores[spot, columns], tall_query) * scale
            ).astype(BF16)
            grads[step - 1][:, pl.ds((groups + group) * HEAD_DIM, HEAD_DIM)] = value_grad(
                probs, spot, ups, group, ratio, rows
            ).astype(BF16)


def backward(partial, ends, inner, query, turned, probs, out_proj, blocks, groups):
    rows, width = query.shape
    heads = width // HEAD_DIM
    reach = len(blocks) - 1
    span = (reach + 1) * rows
    outs = pl.pallas_call(
        functools.partial(backward_kernel, reach=reach, groups=groups),
        in_specs=[WHOLE] * (reach + 5 + 3 * PARTS),
        out_specs=[WHOLE] * (reach + 2),
        out_shape=[pltpu.VMEM((rows, 2 * groups * HEAD_DIM), BF16)] * reach
        + [
            pltpu.VMEM((span, heads * rows), BF16),
            pltpu.VMEM((heads * rows, HEAD_DIM), BF16),
        ],
        scratch_shapes=[pltpu.VMEM((width, rows), BF16)],
        compiler_params=PARAMS,
        cost_estimate=estimate(8 * rows * span * width, 8 * rows * span),
        name="backward",
    )(partial, inner, query, out_proj, *turned, *probs, *ends, *blocks)
    return outs[:reach], outs[reach], outs[reach + 1]


def finish_kernel(scores, ups, query, *refs, reach, groups):
    probs, refs = refs[:PARTS], refs[PARTS:]
    blocks = refs[: reach + 1]
    grad_query, grad = refs[reach + 1 :]
    rows, width = query.shape
    heads = width // HEAD_DIM
    ratio = heads // groups
    scale = HEAD_DIM ** (-0.5)
    spot = pl.ds(0, rows)
    for group in range(groups):
        picked = range(group * ratio, (group + 1) * ratio)
        tall_query = jnp.concatenate([head_of(query, head) for head in picked], 0)
        columns = pl.ds(group * ratio * rows, ratio * rows)
        grad[:, pl.ds(group * HEAD_DIM, HEAD_DIM)] = dot(scores[spot, columns], tall_query) * scale
        grad[:, pl.ds((groups + group) * HEAD_DIM, HEAD_DIM)] = value_grad(
            probs, spot, ups, group, ratio, rows
        )
        keys = jnp.concatenate([head_of(blocks[step], group) for step in range(reach + 1)], 0).T
        for head in picked:
            total = dot(keys, scores[:, pl.ds(head * rows, rows)])
            grad_query[:, pl.ds(head * HEAD_DIM, HEAD_DIM)] = (total * scale).T.astype(BF16)


def finish(scores, ups, query, probs, blocks, groups):
    rows, width = query.shape
    reach = len(blocks) - 1
    span = (reach + 1) * rows
    return pl.pallas_call(
        functools.partial(finish_kernel, reach=reach, groups=groups),
        in_specs=[WHOLE] * (reach + 4 + PARTS),
        out_specs=[WHOLE] * 2,
        out_shape=[
            jax.ShapeDtypeStruct((rows, width), BF16),
            pltpu.VMEM((rows, 2 * groups * HEAD_DIM), F32),
        ],
        compiler_params=PARAMS,
        cost_estimate=estimate(2 * rows * span * width, 4 * rows * span),
        name="finish",
    )(scores, ups, query, *probs, *blocks)


def body(queries, key_vectors, values, out_proj, grad_out, windows, slab_order):
    groups = key_vectors.shape[1] // HEAD_DIM
    devices = lax.axis_size("seq")
    size = lax.axis_size("head")
    assert size == 4 and devices % 4 == 0
    reach = min(8, devices // 2)
    half = reach // 2
    even = lax.axis_index("seq") % 2 == 0
    nothing = jnp.zeros((), BF16)

    across = []
    for i in range(devices):
        for first, second in ((1, (i, 2)), (2, (i, 1)), (0, (i ^ 1, 0)), (3, (i ^ 1, 3))):
            across.append((i * size + first, second[0] * size + second[1]))

    def outer(array):
        return lax.ppermute(array, "head", [(i ^ 1, i) for i in range(size)])

    def inner(array):
        return lax.ppermute(array, ("seq", "head"), across)

    def shifted(array, step):
        pairs = [((i - step) % devices, i) for i in range(devices)]
        return lax.ppermute(array, "seq", pairs)

    def swapped(array):
        return lax.ppermute(array, "seq", [(i ^ 1, i) for i in range(devices)])

    pair, query, limits = stage(key_vectors, values, queries, windows, slab_order, reach)
    fetched = [pair] + [shifted(pair, 2 * step) for step in range(1, half + 1)]
    traded = [swapped(jnp.where(even, pair, fetched[half]))]
    traded += [swapped(fetched[step]) for step in range(1, half)]
    blocks = [pair]
    for step in range(half):
        blocks.append(jnp.where(even, traded[(step + 1) % half], traded[step]))
        blocks.append(fetched[step + 1])

    both = range(PARTS)
    outer1, inner1 = outer(grad_out), inner(grad_out)
    proj = bring(out_proj)
    attention, turned, probs, lead = zip(
        *[forward(limits, query, proj, blocks, part, groups, size) for part in both]
    )
    split1 = split(outer1)
    inner2 = [inner(split1[i]) for i in both]
    rows = lead[0].shape[0]
    send2 = [either(lead[i], inner1, i * rows) for i in both]
    outer2 = [outer(send2[i]) for i in both]
    own_share, partial, far_share, pair_share = middle(attention, grad_out, outer1, proj)
    send3 = [either(far_share[i], inner2[i], 0) for i in both]
    outer3 = [outer(send3[i]) for i in both]
    inner3 = [inner(far_share[i] + outer2[i]) for i in both]
    partial = far(partial, outer2, inner2, proj)
    sent, scores, ups = backward(
        partial, outer3, inner1, query, turned, probs, proj, blocks, groups
    )
    inner4 = [inner(lead[i] + outer3[i]) for i in both]
    outer4 = [outer(carry(pair_share[i], inner3[i])) for i in both]

    taken = [swapped(sent[2 * step]) for step in range(half)]
    total = []
    for step in range(half):
        near = taken[step]
        if step + 1 < half:
            near = jnp.where(even, taken[step + 1], near)
        else:
            near = jnp.where(even, nothing, near)
        total.append(shifted(sent[2 * step + 1] + near, -2 * (step + 1)))
    grad_queries, own = finish(scores, ups, query, probs, blocks, groups)
    own = own + jnp.where(even, taken[0], nothing).astype(F32)
    for part in total:
        own = own + part.astype(F32)
    grad_keys = own[:, : groups * HEAD_DIM].astype(BF16)
    grad_values = own[:, groups * HEAD_DIM :].astype(BF16)
    layer_out = total_of(own_share, *outer4, *inner4)
    return layer_out, grad_queries, grad_keys, grad_values


def solution(mesh):
    in_specs = (
        P("seq", "head"),
        P("seq", "head"),
        P("seq", "head"),
        P("head", None),
        P("seq", "head"),
        P("head"),
        P(),
    )
    out_specs = (P("seq", "head"), P("seq", "head"), P("seq", "head"), P("seq", "head"))
    return jax.shard_map(body, mesh=mesh, in_specs=in_specs, out_specs=out_specs, check_vma=False)
```
